32 devices in a mesh: row: 4 (over x, core), col: 4 (over z), inner: 2 (over y).
Axes of the slice: x: 2, y: 2, z: 4, core: 2. Of those that a mesh axis runs over, the one named last changes fastest.
Arguments:
- near_flags: int32 [4, 6], P('row', 'inner'), may hold values 0 or 1
- row_factor: bfloat16 [4, 6, 64, 2048], P('row', 'inner', None, 'col'), may hold values from -6 to 6
- col_factor: bfloat16 [4, 6, 64, 2048], P('row', 'inner', None, 'col'), may hold values from -0.0068359375 to 0.0068359375
- near_block: bfloat16 [4, 6, 2048, 2048], P('row', 'inner', None, 'col'), may hold values from -0.0546875 to 0.0546875
- inner_left: bfloat16 [6, 16, 64, 2048], P('inner', 'col', None, 'row'), may hold values from -6 to 6
- inner_right: bfloat16 [6, 16, 64, 2048], P('inner', 'col', None, 'row'), may hold values from -0.75 to 0.75
- sketch_matrix: bfloat16 [16, 64, 2048], P('col'), may hold values from -0.125 to 0.125
Outputs:
- basis: float32 [4, 16, 64, 2048], P('row', 'col', None, 'inner')
- coupling: float32 [4, 16, 64, 2048], P('row', 'col', None, 'inner')
The draws below stay inside these ranges and needn't reach their ends.
Inputs may be any that keep to these rules, and one draw needn't show every extreme that they name: `near_flags`: 1 marks a near-field block.
All inputs are finite; a program needn't handle non-finite values.
Results may differ from the reference program's by a relative error of at most 0.0055.
Values may be sent and summed in bfloat16 or wider, within the bound.
A program may use at most 128 MiB of HBM per device.

```python
import math
import jax
import jax.numpy as jnp
from jax import lax

L = 2048
R = 64
K_I = 4
K_J = 16
K_K = 6


def set_ends(values, rng, least, top_value):
    place = [jax.random.randint(jax.random.fold_in(rng, axis), (), 0, length) for axis, length in enumerate(values.shape)]
    main_axis = values.shape.index(max(values.shape))
    next_to = place[:main_axis] + [(place[main_axis] + 1) % values.shape[main_axis]] + place[main_axis + 1:]
    return values.at[tuple(place)].set(least).at[tuple(next_to)].set(top_value)


def level_of(key, dims, split, smallest, high):
    def one(axis_at, parts):
        steps = jax.random.uniform(jax.random.fold_in(jax.random.fold_in(key, 6), axis_at), (parts,), jnp.float32, smallest / len(split), high / len(split))
        return jnp.repeat(jnp.exp(steps), dims[axis_at] // parts).reshape((-1,) + (1,) * (len(dims) - axis_at - 1))

    factor_of = one(*split[0])
    for cut in split[1:]:
        factor_of = factor_of * one(*cut)
    return factor_of


def scatter_about(rng, dims, scale, bound, cuts=(), dtype=jnp.bfloat16):
    drawn = jax.random.normal(rng, dims, jnp.float32) * scale
    if len(cuts) > 0:
        drawn = level_of(rng, dims, cuts, -0.22, 0.18) * drawn
    return jnp.clip(drawn, min=-bound, max=bound).astype(dtype)


def setup_inputs(seed: int = 0) -> dict:
    splits = jax.random.split(jax.random.key(seed), 8)
    near_flags = set_ends((jax.random.randint(splits[0], (K_I, K_K), 0, 2) < 1).astype(jnp.int32), jax.random.fold_in(splits[0], 1), 0, 1)
    row_factor = scatter_about(splits[1], (K_I, K_K, R, L), 1.0, 6.0, ((0, 4), (1, 2), (3, 4)))
    col_factor = scatter_about(splits[2], (K_I, K_K, R, L), (R * L * K_K) ** -0.5, 0.0068359375, ((0, 4), (1, 2), (3, 4)))
    near_block = scatter_about(splits[3], (K_I, K_K, L, L), (L * K_K) ** -0.5, 0.0546875, ((0, 4), (1, 2), (3, 4)))
    inner_left = scatter_about(splits[4], (K_K, K_J, R, L), 1.0, 6.0, ((0, 2), (1, 4), (3, 4)))
    inner_right = scatter_about(splits[5], (K_K, K_J, R, L), R ** -0.5, 0.75, ((0, 2), (1, 4), (3, 4)))
    sketch_matrix = scatter_about(splits[6], (K_J, R, L), L ** -0.5, 0.125, ((0, 4),))
    return dict(near_flags=near_flags, row_factor=row_factor, col_factor=col_factor, near_block=near_block, inner_left=inner_left, inner_right=inner_right, sketch_matrix=sketch_matrix)


def solve_lower(lower, sampled):
    return jax.scipy.linalg.solve_triangular(lower, sampled, lower=True)

def reference(near_flags, row_factor, col_factor, near_block, inner_left, inner_right, sketch_matrix):
    wide = jnp.float32
    narrow = jnp.bfloat16
    highest = lax.Precision.HIGHEST
    reduced = jnp.einsum('kjrl,jsl->kjrs', inner_right.astype(wide), sketch_matrix.astype(wide)).astype(narrow)
    right_wide = inner_right.astype(wide)

    def block_row(operands):
        rows_i, cols_i, dense_i, flags_i = operands

        def one_block(inner_ops):
            rows_k, cols_k, dense_k, flag_k, left_k = inner_ops

            def lowrank(unused):
                coupled = jnp.einsum('rl,jsl->jrs', cols_k.astype(wide), left_k.astype(wide)).astype(narrow)
                return jnp.einsum('jrs,rl->jsl', coupled.astype(wide), rows_k.astype(wide))

            def neardense(unused):
                flat = left_k.reshape(K_J * R, L)
                return jnp.dot(flat, dense_k, preferred_element_type=wide).reshape(K_J, R, L)
            return lax.cond(flag_k > 0, neardense, lowrank, 0).astype(narrow)
        pieces = lax.map(one_block, (rows_i, cols_i, dense_i, flags_i, inner_left))
        pieces_wide = pieces.astype(wide)
        sampled = jnp.einsum('kjrs,kjrl->jsl', reduced.astype(wide), pieces_wide)
        gram_matrix = jnp.einsum('jsl,jtl->jst', sampled, sampled, precision=highest) / L
        lower = jnp.linalg.cholesky(gram_matrix)
        basis = jax.vmap(solve_lower)(lower, sampled)
        projected = jnp.einsum('kjrl,jsl->kjrs', pieces_wide, basis, precision=highest) / math.sqrt(L)
        coupling = jnp.einsum('kjrs,kjrl->jsl', projected, right_wide, precision=highest)
        return (basis, coupling)
    basis, coupling = lax.map(block_row, (row_factor, col_factor, near_block, near_flags))
    return (basis, coupling)
```

```python
import functools
import math

import jax
import jax.numpy as jnp
from jax import lax
from jax.experimental import pallas as pl
from jax.experimental.pallas import tpu as pltpu
from jax.sharding import PartitionSpec as P

MESH = pl.DeviceIdType.MESH
HIGHEST = lax.Precision.HIGHEST
WIDE = jnp.float32
NARROW = jnp.bfloat16


def remote(src, dst, sems, slot, device):
    return pltpu.make_async_remote_copy(
        src_ref=src, dst_ref=dst, send_sem=sems[0].at[slot], recv_sem=sems[1].at[slot],
        device_id=device, device_id_type=MESH,
    )


def meet(devices):
    barrier = pltpu.get_barrier_semaphore()
    for device in devices:
        pl.semaphore_signal(barrier, inc=1, device_id=device, device_id_type=MESH)
    pl.semaphore_wait(barrier, len(devices))


def gather_kernel(dims, left_ref, right_ref, cols_ref, xg, yg, yi, vg, send, recv, own):
    n_row, n_col, n_in, slots, js, width, cols = dims
    share = yi.shape[-1]
    row, col, inner = lax.axis_index("row"), lax.axis_index("col"), lax.axis_index("inner")
    twin_row = row + 1 - 2 * lax.rem(row, 2)
    far_row = lax.rem(row + 2, n_row)
    twin_far = lax.rem(twin_row + 2, n_row)
    sems = (send, recv)
    twin = {"row": twin_row}
    far = {"row": far_row}
    up = {"col": lax.rem(col + 1, n_col)}
    down = {"col": lax.rem(col + n_col - 1, n_col)}
    col_peers = [{"col": lax.rem(col + d, n_col)} for d in range(1, n_col)]
    inner_peers = [lax.rem(inner + d, n_in) for d in range(1, n_in)]
    meet([twin, far] + col_peers + [{"inner": p} for p in inner_peers])

    started = []

    def push(src, dst, device):
        copy = remote(src, dst, sems, len(started), device)
        copy.start()
        started.append(copy)
        return copy

    def place(k, r, c, part=None):
        first, length = (0, js) if part is None else (part * (js // 2), js // 2)
        return xg.at[
            k,
            pl.ds(pl.multiple_of(c * js + first, js // 2), length),
            pl.ds(pl.multiple_of(r * width, width), width),
        ]

    def y_place(r):
        return yg.at[:, :, pl.ds(pl.multiple_of(r * width, width), width)]

    def v_place(c):
        return vg.at[:, :, pl.ds(pl.multiple_of(c * cols, cols), cols)]

    half = n_col // 2
    y_far = push(right_ref, y_place(row), far)
    y_twin = push(right_ref, y_place(row), twin)
    v_copies = [push(cols_ref, v_place(col), peer) for peer in col_peers]
    far_got = []
    rings = {}
    twin_copies = []
    for k in range(slots):
        mine = left_ref.at[k]
        spot = place(k, row, col)
        far_got.append(push(mine, spot, far))
        rings[0, 1, k] = (push(mine, spot, up), push(mine, spot, down))
        twin_copies.append(push(mine, spot, twin))
    local_x = [pltpu.make_async_copy(left_ref.at[k], place(k, row, col), own.at[k]) for k in range(slots)]
    local_y = pltpu.make_async_copy(right_ref, y_place(row), own.at[slots])
    local_v = pltpu.make_async_copy(cols_ref, v_place(col), own.at[slots + 1])
    local_y.start()
    local_v.start()
    for copy in local_x:
        copy.start()
    y_far.wait_recv()
    y_twin_far = push(y_place(far_row), y_place(far_row), twin)
    rows = (row, far_row)
    for k in range(slots):
        far_got[k].wait_recv()
        spot = place(k, far_row, col)
        rings[1, 1, k] = (push(spot, spot, up), push(spot, spot, down))
        twin_copies.append(push(spot, spot, twin))
    local_y.wait()
    y_twin.wait_recv()
    y_twin_far.wait_recv()
    y_out = []
    for peer in inner_peers:
        src = yg.at[:, :, pl.ds(pl.multiple_of(peer * share, share), share)]
        y_out.append(push(src, yi.at[inner], {"inner": peer}))
    local_i = pltpu.make_async_copy(
        yg.at[:, :, pl.ds(pl.multiple_of(inner * share, share), share)], yi.at[inner], own.at[slots + 2]
    )
    local_i.start()
    for step in range(1, half + 1):
        for stream in range(2):
            for k in range(slots):
                got_up, got_down = rings[stream, step, k]
                from_up = lax.rem(col + n_col - step, n_col)
                from_down = lax.rem(col + step, n_col)
                parts = (None, None) if step < half else (0, 1)
                got_up.wait_recv()
                a = place(k, rows[stream], from_up, parts[0])
                if step < half:
                    last = step + 1 == half
                    a_next = place(k, rows[stream], from_up, 0) if last else a
                    next_up = push(a_next, a_next, up)
                twin_copies.append(push(a, a, twin))
                got_down.wait_recv()
                b = place(k, rows[stream], from_down, parts[1])
                if step < half:
                    b_next = place(k, rows[stream], from_down, 1) if last else b
                    next_down = push(b_next, b_next, down)
                    rings[stream, step + 1, k] = (next_up, next_down)
                twin_copies.append(push(b, b, twin))
    for copy in twin_copies + v_copies + y_out:
        copy.wait_recv()
    for copy in local_x + [local_v, local_i]:
        copy.wait()
    for copy in started:
        copy.wait_send()


def gather_all(left, right, cols_own, sizes):
    n_row, n_col, n_in = sizes
    slots, js, width = left.shape
    rank, cols = cols_own.shape[1:]
    total = width * n_row
    half = n_col // 2
    n_copies = 3 + (n_col - 1) + (n_in - 1) + slots * (4 + 3 + 2 * (2 * half + 2 * (half - 1)))
    dims = (n_row, n_col, n_in, slots, js, width, cols)
    any_spec = pl.BlockSpec(memory_space=pltpu.HBM)
    return pl.pallas_call(
        functools.partial(gather_kernel, dims),
        out_shape=(
            jax.ShapeDtypeStruct((slots, n_col * js, total), left.dtype),
            jax.ShapeDtypeStruct((slots, js, total), left.dtype),
            jax.ShapeDtypeStruct((n_in, slots, js, total // n_in), left.dtype),
            jax.ShapeDtypeStruct((slots, rank, total), left.dtype),
        ),
        in_specs=[any_spec] * 3,
        out_specs=[any_spec] * 4,
        scratch_shapes=[
            pltpu.SemaphoreType.DMA((n_copies,)),
            pltpu.SemaphoreType.DMA((n_copies,)),
            pltpu.SemaphoreType.DMA((slots + 3,)),
        ],
        compiler_params=pltpu.CompilerParams(collective_id=0, has_side_effects=True),
    )(left, right, cols_own)


def spread_kernel(dims, p_ref, z_ref, pr, zr, send, recv, zsend, zrecv, own):
    n_col, n_in, group = dims
    col, inner = lax.axis_index("col"), lax.axis_index("inner")
    home = lax.div(col, group)
    slot = lax.rem(col, group)
    meets = []
    targets = []
    for d in range(n_col):
        targets.append({"col": lax.rem(col + d, n_col), "inner": home})
    peers = [lax.rem(inner + d, n_in) for d in range(1, n_in)]
    barrier = pltpu.get_barrier_semaphore()
    n_all = 0
    for d in range(n_col):
        for e in range(n_in):
            if d or e:
                pl.semaphore_signal(
                    barrier, inc=1,
                    device_id={"col": lax.rem(col + d, n_col), "inner": lax.rem(inner + e, n_in)},
                    device_id_type=MESH,
                )
                n_all += 1
    pl.semaphore_wait(barrier, n_all)
    z_copies = []
    for e, peer in enumerate(peers):
        copy = remote(z_ref, zr.at[inner], (zsend, zrecv), e, {"inner": peer})
        copy.start()
        z_copies.append(copy)
    z_own = pltpu.make_async_copy(z_ref, zr.at[inner], own.at[1])
    z_own.start()

    def block(d):
        return pltpu.make_async_remote_copy(
            src_ref=p_ref.at[lax.rem(col + d, n_col)], dst_ref=pr.at[inner, slot],
            send_sem=send.at[d], recv_sem=recv.at[inner, slot],
            device_id=targets[d], device_id_type=MESH,
        )

    for d in range(1, n_col):
        block(d).start()

    @pl.when(home != inner)
    def _():
        block(0).start()

    @pl.when(home == inner)
    def _():
        pltpu.make_async_copy(p_ref.at[col], pr.at[inner, slot], own.at[0]).start()

    for e in range(n_in):
        for g in range(group):
            is_own = jnp.logical_and(inner == e, col == inner * group + g)

            @pl.when(jnp.logical_not(is_own))
            def _(e=e, g=g):
                pltpu.make_async_remote_copy(
                    src_ref=p_ref.at[0], dst_ref=pr.at[e, g], send_sem=send.at[0], recv_sem=recv.at[e, g],
                    device_id=targets[1], device_id_type=MESH,
                ).wait_recv()

    @pl.when(home == inner)
    def _():
        pltpu.make_async_copy(p_ref.at[col], pr.at[inner, slot], own.at[0]).wait()

    @pl.when(home != inner)
    def _():
        block(0).wait_send()

    for d in range(1, n_col):
        block(d).wait_send()
    z_own.wait()
    for copy in z_copies:
        copy.wait()


def spread(p, z, sizes):
    n_row, n_col, n_in = sizes
    group = n_col // n_in
    vmem = pl.BlockSpec(memory_space=pltpu.VMEM)
    return pl.pallas_call(
        functools.partial(spread_kernel, (n_col, n_in, group)),
        out_shape=(
            jax.ShapeDtypeStruct((n_in, group) + p.shape[1:], p.dtype),
            jax.ShapeDtypeStruct((n_in,) + z.shape, z.dtype),
        ),
        in_specs=[vmem, vmem],
        out_specs=[vmem, vmem],
        scratch_shapes=[
            pltpu.SemaphoreType.DMA((n_col,)),
            pltpu.SemaphoreType.DMA((n_in, group)),
            pltpu.SemaphoreType.DMA((n_in,)),
            pltpu.SemaphoreType.DMA((n_in,)),
            pltpu.SemaphoreType.DMA((2,)),
        ],
        compiler_params=pltpu.CompilerParams(collective_id=1, has_side_effects=True),
    )(p, z)


def total_kernel(n_in, part_ref, out_ref, got, send, recv):
    inner = lax.axis_index("inner")
    peers = [lax.rem(inner + d, n_in) for d in range(1, n_in)]
    meet([{"inner": peer} for peer in peers])
    copies = []
    for e, peer in enumerate(peers):
        copy = remote(part_ref, got.at[e], (send, recv), e, {"inner": peer})
        copy.start()
        copies.append(copy)
    for copy in copies:
        copy.wait()
    out = part_ref[...]
    for e in range(n_in - 1):
        out = out + got[e]
    out_ref[...] = out


def total_over_inner(part, n_in):
    vmem = pl.BlockSpec(memory_space=pltpu.VMEM)
    return pl.pallas_call(
        functools.partial(total_kernel, n_in),
        out_shape=jax.ShapeDtypeStruct(part.shape, part.dtype),
        in_specs=[vmem],
        out_specs=vmem,
        scratch_shapes=[
            pltpu.VMEM((n_in - 1,) + part.shape, part.dtype),
            pltpu.SemaphoreType.DMA((n_in - 1,)),
            pltpu.SemaphoreType.DMA((n_in - 1,)),
        ],
        compiler_params=pltpu.CompilerParams(collective_id=2, has_side_effects=True),
    )(part)


def inverse_factor_kernel(g_ref, out_ref):
    count, size, _ = g_ref.shape
    tall = lax.broadcasted_iota(jnp.int32, (size, size), 0)
    wide = lax.broadcasted_iota(jnp.int32, (size, size), 1)
    eye = (tall == wide).astype(WIDE)
    lines = lax.broadcasted_iota(jnp.int32, (8, 1), 0)
    works = []
    for j in range(count):
        full = jnp.concatenate([g_ref[j], eye], axis=1)
        works.append([full[8 * b : 8 * b + 8] for b in range(size // 8)])
    scales = [[] for _ in range(count)]
    for k in range(size):
        b0, in_b = k // 8, k % 8
        for j in range(count):
            work = works[j]
            line = work[b0][in_b : in_b + 1]
            pivot = line[:, k : k + 1]
            scales[j].append(lax.rsqrt(pivot))
            line = line * (1.0 / pivot)
            for b in range(b0, size // 8):
                column = work[b][:, k : k + 1]
                if b == b0:
                    if in_b == 7:
                        continue
                    column = jnp.where(lines > in_b, column, 0.0)
                work[b] = work[b] - column * line
    for j in range(count):
        scale = jnp.concatenate(scales[j], axis=0)
        out_ref[j] = jnp.concatenate(works[j], axis=0)[:, size:] * scale


def inverse_factor(gram):
    vmem = pl.BlockSpec(memory_space=pltpu.VMEM)
    return pl.pallas_call(
        inverse_factor_kernel,
        out_shape=jax.ShapeDtypeStruct(gram.shape, gram.dtype),
        in_specs=[vmem],
        out_specs=vmem,
    )(gram)


def local(sizes, near_flags, row_factor, col_factor, near_block, inner_left, inner_right, sketch_matrix):
    n_row, n_col, n_in = sizes
    slots, own_j, rank, width = inner_left.shape
    js = own_j * rank
    total = width * n_row
    cols = total // n_col
    share = total // n_in
    xg, yg, yi, vg = gather_all(
        inner_left.reshape(slots, js, width), inner_right.reshape(slots, js, width), col_factor[0], sizes
    )
    nearness = near_flags[0]
    pieces = []
    for slot in range(slots):

        def lowrank(slot=slot):
            coupled = lax.dot_general(
                xg[slot], vg[slot], (((1,), (1,)), ((), ())), preferred_element_type=WIDE
            ).astype(NARROW)
            return jnp.dot(coupled, row_factor[0, slot], preferred_element_type=WIDE).astype(NARROW)

        def neardense(slot=slot):
            return jnp.dot(xg[slot], near_block[0, slot], preferred_element_type=WIDE).astype(NARROW)

        pieces.append(lax.cond(nearness[slot] > 0, neardense, lowrank))
    spread_out = jnp.stack([p.reshape(n_col, js, cols) for p in pieces], axis=1)
    reduced = jnp.einsum(
        "kjrl,jsl->krjs", yg.reshape(slots, own_j, rank, total), sketch_matrix, preferred_element_type=WIDE
    ).astype(NARROW)
    got, reduced_all = spread(spread_out, reduced.reshape(slots * rank, js), sizes)
    group = n_col // n_in
    stacked = got.reshape(n_in, group, slots, own_j, rank, cols).transpose(3, 0, 2, 4, 1, 5)
    stacked = stacked.reshape(own_j, n_in * slots * rank, share)
    z_all = reduced_all.reshape(n_in * slots * rank, own_j, rank)
    sampled = jnp.einsum("ajs,jal->jsl", z_all, stacked, preferred_element_type=WIDE)
    high = sampled.astype(NARROW)
    low = (sampled - high.astype(WIDE)).astype(NARROW)
    both = jnp.concatenate([high, low], axis=1)
    cross = jnp.einsum("jsl,jal->jsa", both, stacked, preferred_element_type=WIDE)
    cross = cross[:, :rank] + cross[:, rank:]
    gram = jnp.einsum("jsl,jtl->jst", sampled, sampled, precision=HIGHEST) / total
    summed = total_over_inner(jnp.concatenate([cross, gram], axis=2), n_in)
    depth = n_in * slots * rank
    inverse = inverse_factor(summed[:, :, depth:])
    basis = jnp.einsum("jst,jtl->jsl", inverse, sampled, precision=HIGHEST)
    projected = jnp.einsum("jst,jta->jsa", inverse, summed[:, :, :depth], precision=HIGHEST) / math.sqrt(total)
    p_high = projected.astype(NARROW)
    p_low = (projected - p_high.astype(WIDE)).astype(NARROW)
    yk = yi.reshape(n_in * slots, own_j, rank, share)
    p_both = jnp.concatenate([p_high, p_low], axis=1).reshape(own_j, 2 * rank, n_in * slots, rank)
    coupling = jnp.einsum("jskr,kjrl->jsl", p_both, yk, preferred_element_type=WIDE)
    coupling = coupling[:, :rank] + coupling[:, rank:]
    return (basis[None], coupling[None])


def solution(mesh):
    sizes = (mesh.shape["row"], mesh.shape["col"], mesh.shape["inner"])
    in_specs = (
        P("row", "inner"),
        P("row", "inner", None, "col"),
        P("row", "inner", None, "col"),
        P("row", "inner", None, "col"),
        P("inner", "col", None, "row"),
        P("inner", "col", None, "row"),
        P("col", None, None),
    )
    out_specs = (P("row", "col", None, "inner"), P("row", "col", None, "inner"))
    return jax.shard_map(
        functools.partial(local, sizes), mesh=mesh, in_specs=in_specs, out_specs=out_specs, check_vma=False
    )
```

```python
import functools
import math

import jax
import jax.numpy as jnp
from jax import lax
from jax.experimental import pallas as pl
from jax.experimental.pallas import tpu as pltpu
from jax.sharding import PartitionSpec as P

MESH = pl.DeviceIdType.MESH
HIGHEST = lax.Precision.HIGHEST
WIDE = jnp.float32
NARROW = jnp.bfloat16


def remote(src, dst, sems, slot, device):
    return pltpu.make_async_remote_copy(
        src_ref=src, dst_ref=dst, send_sem=sems[0].at[slot], recv_sem=sems[1].at[slot],
        device_id=device, device_id_type=MESH,
    )


def meet(devices):
    barrier = pltpu.get_barrier_semaphore()
    for device in devices:
        pl.semaphore_signal(barrier, inc=1, device_id=device, device_id_type=MESH)
    pl.semaphore_wait(barrier, len(devices))


def gather_kernel(dims, left_ref, right_ref, cols_ref, xg, yg, yi, vg, stage, send, recv, own):
    n_row, n_col, n_in, slots, js, width, rank, cols = dims
    share = yi.shape[-1]
    row, col, inner = lax.axis_index("row"), lax.axis_index("col"), lax.axis_index("inner")
    twin_row = row + 1 - 2 * lax.rem(row, 2)
    far_row = lax.rem(row + 2, n_row)
    sems = (send, recv)
    twin = {"row": twin_row}
    far = {"row": far_row}
    up = {"col": lax.rem(col + 1, n_col)}
    down = {"col": lax.rem(col + n_col - 1, n_col)}
    inner_peers = [lax.rem(inner + d, n_in) for d in range(1, n_in)]
    meet([twin, far, up, down] + [{"inner": p} for p in inner_peers])

    started = []

    def push(src, dst, device):
        copy = remote(src, dst, sems, len(started), device)
        copy.start()
        started.append(copy)
        return copy

    def x_place(r):
        def place(k, c, part=None):
            first, length = (0, js) if part is None else (part * (js // 2), js // 2)
            return xg.at[
                k,
                pl.ds(pl.multiple_of(c * js + first, js // 2), length),
                pl.ds(pl.multiple_of(r * width, width), width),
            ]

        return place

    def y_place(r):
        return yg.at[:, :, pl.ds(pl.multiple_of(r * width, width), width)]

    def v_place(k, c, part=None):
        rows = pl.ds(0, rank) if part is None else pl.ds(part * (rank // 2), rank // 2)
        return vg.at[:, rows, pl.ds(pl.multiple_of(c * cols, cols), cols)]

    half = n_col // 2
    twins = []

    def ring_start(src, place, k):
        spot = place(k, col)
        return (push(src, spot, up), push(src, spot, down))

    def ring_step(pair, place, k, step, relay):
        got_up, got_down = pair
        from_up = lax.rem(col + n_col - step, n_col)
        from_down = lax.rem(col + step, n_col)
        nexts = []
        for got, source, device, part in ((got_up, from_up, up, 0), (got_down, from_down, down, 1)):
            got.wait_recv()
            here = place(k, source, None if step < half else part)
            if step < half:
                on = place(k, source, part) if step + 1 == half else here
                nexts.append(push(on, on, device))
            if relay:
                twins.append(push(here, here, twin))
        return tuple(nexts)

    near, other = x_place(row), x_place(far_row)
    y_far = push(right_ref, y_place(row), far)
    near_rings, far_got = [], []
    for k in range(slots):
        near_rings.append(ring_start(left_ref.at[k], near, k))
        far_got.append(push(left_ref.at[k], near(k, col), far))
    v_ring = ring_start(cols_ref, v_place, 0)
    y_twin = push(right_ref, y_place(row), twin)
    for k in range(slots):
        twins.append(push(left_ref.at[k], near(k, col), twin))
    locals_ = [pltpu.make_async_copy(left_ref.at[k], near(k, col), own.at[k]) for k in range(slots)]
    local_y = pltpu.make_async_copy(right_ref, y_place(row), own.at[slots])
    locals_.append(pltpu.make_async_copy(cols_ref, v_place(0, col), own.at[slots + 1]))
    local_y.start()
    for copy in locals_:
        copy.start()
    for k in range(slots):
        near_rings[k] = ring_step(near_rings[k], near, k, 1, True)
    y_far.wait_recv()
    y_twin_far = push(y_place(far_row), y_place(far_row), twin)
    far_rings, y_out = [], []
    for k in range(slots):
        far_got[k].wait_recv()
        spot = other(k, col)
        far_rings.append(ring_start(spot, other, k))
        twins.append(push(spot, spot, twin))
        if k == 0:
            local_y.wait()
            y_twin.wait_recv()
            y_twin_far.wait_recv()
            for peer in inner_peers:
                src = yg.at[:, :, pl.ds(pl.multiple_of(peer * share, share), share)]
                y_out.append(push(src, yi.at[inner], {"inner": peer}))
            fetch = pltpu.make_async_copy(
                yg.at[:, :, pl.ds(pl.multiple_of(inner * share, share), share)], stage, own.at[slots + 2]
            )
            fetch.start()
    v_ring = ring_step(v_ring, v_place, 0, 1, False)
    fetch.wait()
    store = pltpu.make_async_copy(stage, yi.at[inner], own.at[slots + 3])
    store.start()
    for k in range(slots):
        far_rings[k] = ring_step(far_rings[k], other, k, 1, True)
    for step in range(2, half + 1):
        for k in range(slots):
            near_rings[k] = ring_step(near_rings[k], near, k, step, True)
        v_ring = ring_step(v_ring, v_place, 0, step, False)
        for k in range(slots):
            far_rings[k] = ring_step(far_rings[k], other, k, step, True)
    for copy in twins + y_out:
        copy.wait_recv()
    for copy in locals_ + [store]:
        copy.wait()
    for copy in started:
        copy.wait_send()


def gather_all(left, right, cols_own, sizes):
    n_row, n_col, n_in = sizes
    slots, js, width = left.shape
    rank, cols = cols_own.shape[1:]
    total = width * n_row
    half = n_col // 2
    n_copies = 3 + (n_in - 1) + slots * 3 + (2 * slots + 1) * 2 * half + 2 * slots * 2 * half
    dims = (n_row, n_col, n_in, slots, js, width, rank, cols)
    hbm = pl.BlockSpec(memory_space=pltpu.HBM)
    vmem = pl.BlockSpec(memory_space=pltpu.VMEM)
    return pl.pallas_call(
        functools.partial(gather_kernel, dims),
        out_shape=(
            jax.ShapeDtypeStruct((slots, n_col * js, total), left.dtype),
            jax.ShapeDtypeStruct((slots, js, total), left.dtype),
            jax.ShapeDtypeStruct((n_in, slots, js, total // n_in), left.dtype),
            jax.ShapeDtypeStruct((slots, rank, total), left.dtype),
        ),
        in_specs=[vmem] * 3,
        out_specs=[hbm] * 4,
        scratch_shapes=[
            pltpu.VMEM((slots, js, total // n_in), left.dtype),
            pltpu.SemaphoreType.DMA((n_copies,)),
            pltpu.SemaphoreType.DMA((n_copies,)),
            pltpu.SemaphoreType.DMA((slots + 4,)),
        ],
        compiler_params=pltpu.CompilerParams(collective_id=0, has_side_effects=True),
    )(left, right, cols_own)


def spread_kernel(dims, p_ref, z_ref, pr, zr, relay, send, recv, hop_send, hop_recv, on_send, on_recv, zsend, zrecv, own):
    n_col, n_in, group, own_j, cols = dims
    col, inner = lax.axis_index("col"), lax.axis_index("inner")
    half, half_j = n_col // 2, own_j // 2

    def home(c):
        return lax.div(c, group)

    def column(d):
        return lax.rem(col + n_col + d, n_col)

    def window(c, first=0, length=own_j):
        at = pl.multiple_of(lax.rem(c, group) * cols, cols)
        return pr.at[pl.ds(first, length), inner, :, :, pl.ds(at, cols)]

    meet([
        {"col": column(d), "inner": lax.rem(inner + e, n_in)}
        for d in range(n_col) for e in range(n_in) if d or e
    ])
    sides = (1, -1)
    hops = []
    for n, side in enumerate(sides):
        hop = remote(
            p_ref.at[column(half), pl.ds(n * half_j, half_j)], relay.at[n], (hop_send, hop_recv), n,
            {"col": column(side)},
        )
        hop.start()
        hops.append(hop)

    def block(d):
        return pltpu.make_async_remote_copy(
            src_ref=p_ref.at[column(d)], dst_ref=window(col),
            send_sem=send.at[d], recv_sem=recv.at[inner, lax.rem(col, group)],
            device_id={"col": column(d), "inner": home(col)}, device_id_type=MESH,
        )

    mine = pltpu.make_async_copy(p_ref.at[col], window(col), own.at[0])
    others = [d for d in range(1, n_col) if d != half]
    for d in others:
        block(d).start()

    @pl.when(home(col) != inner)
    def _():
        block(0).start()

    @pl.when(home(col) == inner)
    def _():
        mine.start()

    z_copies = []
    for e in range(1, n_in):
        copy = remote(z_ref, zr.at[inner], (zsend, zrecv), e - 1, {"inner": lax.rem(inner + e, n_in)})
        copy.start()
        z_copies.append(copy)
    z_own = pltpu.make_async_copy(z_ref, zr.at[inner], own.at[1])
    z_own.start()

    ons = []
    for n, side in enumerate(sides):
        hops[n].wait_recv()
        source = column(-side)
        on = pltpu.make_async_remote_copy(
            src_ref=relay.at[n], dst_ref=window(source, n * half_j, half_j),
            send_sem=on_send.at[n], recv_sem=on_recv.at[n, inner],
            device_id={"col": column(half - side), "inner": home(source)}, device_id_type=MESH,
        )
        on.start()
        ons.append(on)

    for e in range(n_in):
        for g in range(group):
            source = inner * group + g
            tied = source == column(half)
            is_own = jnp.logical_and(inner == e, col == source)

            @pl.when(tied)
            def _(e=e):
                for n in range(2):
                    pltpu.make_async_remote_copy(
                        src_ref=relay.at[n], dst_ref=relay.at[n],
                        send_sem=on_send.at[n], recv_sem=on_recv.at[n, e],
                        device_id={"col": column(1), "inner": inner}, device_id_type=MESH,
                    ).wait_recv()

            @pl.when(jnp.logical_not(jnp.logical_or(tied, is_own)))
            def _(e=e, g=g):
                pltpu.make_async_remote_copy(
                    src_ref=p_ref.at[0], dst_ref=p_ref.at[0], send_sem=send.at[0], recv_sem=recv.at[e, g],
                    device_id={"col": column(1), "inner": inner}, device_id_type=MESH,
                ).wait_recv()

    @pl.when(home(col) == inner)
    def _():
        mine.wait()

    @pl.when(home(col) != inner)
    def _():
        block(0).wait_send()

    for d in others:
        block(d).wait_send()
    for copy in hops + ons:
        copy.wait_send()
    z_own.wait()
    for copy in z_copies:
        copy.wait()


def spread(p, z, sizes):
    n_row, n_col, n_in = sizes
    group = n_col // n_in
    own_j, slots, rank, cols = p.shape[1:]
    vmem = pl.BlockSpec(memory_space=pltpu.VMEM)
    return pl.pallas_call(
        functools.partial(spread_kernel, (n_col, n_in, group, own_j, cols)),
        out_shape=(
            jax.ShapeDtypeStruct((own_j, n_in, slots, rank, group * cols), p.dtype),
            jax.ShapeDtypeStruct((n_in,) + z.shape, z.dtype),
        ),
        in_specs=[vmem, vmem],
        out_specs=[vmem, vmem],
        scratch_shapes=[
            pltpu.VMEM((2, own_j // 2, slots, rank, cols), p.dtype),
            pltpu.SemaphoreType.DMA((n_col,)),
            pltpu.SemaphoreType.DMA((n_in, group)),
            pltpu.SemaphoreType.DMA((2,)),
            pltpu.SemaphoreType.DMA((2,)),
            pltpu.SemaphoreType.DMA((2,)),
            pltpu.SemaphoreType.DMA((2, n_in)),
            pltpu.SemaphoreType.DMA((n_in,)),
            pltpu.SemaphoreType.DMA((n_in,)),
            pltpu.SemaphoreType.DMA((2,)),
        ],
        compiler_params=pltpu.CompilerParams(collective_id=1, has_side_effects=True),
    )(p, z)


def factor_kernel(n_in, gram_ref, cross_ref, inv_ref, out_ref, gram_got, cross_got, send, recv, csend, crecv):
    inner = lax.axis_index("inner")
    peers = [lax.rem(inner + d, n_in) for d in range(1, n_in)]
    meet([{"inner": peer} for peer in peers])
    grams = [remote(gram_ref, gram_got.at[e], (send, recv), e, {"inner": p}) for e, p in enumerate(peers)]
    crosses = [remote(cross_ref, cross_got.at[e], (csend, crecv), e, {"inner": p}) for e, p in enumerate(peers)]
    for copy in grams + crosses:
        copy.start()
    for copy in grams:
        copy.wait()
    gram = gram_ref[...]
    for e in range(n_in - 1):
        gram = gram + gram_got[e]
    inverse_factor(gram, inv_ref)
    for copy in crosses:
        copy.wait()
    cross = cross_ref[...]
    for e in range(n_in - 1):
        cross = cross + cross_got[e]
    out_ref[...] = cross


def factor_over_inner(gram, cross, n_in):
    vmem = pl.BlockSpec(memory_space=pltpu.VMEM)
    return pl.pallas_call(
        functools.partial(factor_kernel, n_in),
        out_shape=(
            jax.ShapeDtypeStruct(gram.shape, gram.dtype),
            jax.ShapeDtypeStruct(cross.shape, cross.dtype),
        ),
        in_specs=[vmem, vmem],
        out_specs=[vmem, vmem],
        scratch_shapes=[
            pltpu.VMEM((n_in - 1,) + gram.shape, gram.dtype),
            pltpu.VMEM((n_in - 1,) + cross.shape, cross.dtype),
        ] + [pltpu.SemaphoreType.DMA((n_in - 1,))] * 4,
        compiler_params=pltpu.CompilerParams(collective_id=2, has_side_effects=True),
    )(gram, cross)


def inverse_factor(gram, out_ref):
    count, size, _ = gram.shape
    tall = lax.broadcasted_iota(jnp.int32, (size, size), 0)
    wide = lax.broadcasted_iota(jnp.int32, (size, size), 1)
    eye = (tall == wide).astype(WIDE)
    lines = lax.broadcasted_iota(jnp.int32, (8, 1), 0)
    works = []
    for j in range(count):
        full = jnp.concatenate([gram[j], eye], axis=1)
        works.append([full[8 * b : 8 * b + 8] for b in range(size // 8)])
    scales = [[] for _ in range(count)]
    for k in range(size):
        b0, in_b = k // 8, k % 8
        for j in range(count):
            work = works[j]
            line = work[b0][in_b : in_b + 1]
            pivot = line[:, k : k + 1]
            scales[j].append(lax.rsqrt(pivot))
            line = line * (1.0 / pivot)
            for b in range(b0, size // 8):
                column = work[b][:, k : k + 1]
                if b == b0:
                    if in_b == 7:
                        continue
                    column = jnp.where(lines > in_b, column, 0.0)
                work[b] = work[b] - column * line
    for j in range(count):
        scale = jnp.concatenate(scales[j], axis=0)
        out_ref[j] = jnp.concatenate(works[j], axis=0)[:, size:] * scale


def local(sizes, near_flags, row_factor, col_factor, near_block, inner_left, inner_right, sketch_matrix):
    n_row, n_col, n_in = sizes
    slots, own_j, rank, width = inner_left.shape
    js = own_j * rank
    total = width * n_row
    cols = total // n_col
    share = total // n_in
    xg, yg, yi, vg = gather_all(
        inner_left.reshape(slots, js, width), inner_right.reshape(slots, js, width), col_factor[0], sizes
    )
    nearness = near_flags[0]
    pieces = []
    for slot in range(slots):

        def lowrank(slot=slot):
            coupled = lax.dot_general(
                xg[slot], vg[slot], (((1,), (1,)), ((), ())), preferred_element_type=WIDE
            ).astype(NARROW)
            return jnp.dot(coupled, row_factor[0, slot], preferred_element_type=WIDE).astype(NARROW)

        def neardense(slot=slot):
            return jnp.dot(xg[slot], near_block[0, slot], preferred_element_type=WIDE).astype(NARROW)

        pieces.append(lax.cond(nearness[slot] > 0, neardense, lowrank))
    spread_out = jnp.stack([p.reshape(n_col, own_j, rank, cols) for p in pieces], axis=2)
    reduced = jnp.einsum(
        "kjrl,jsl->krjs", yg.reshape(slots, own_j, rank, total), sketch_matrix, preferred_element_type=WIDE
    ).astype(NARROW)
    got, reduced_all = spread(spread_out, reduced.reshape(slots * rank, js), sizes)
    stacked = got.reshape(own_j, n_in * slots * rank, share)
    z_all = reduced_all.reshape(n_in * slots * rank, own_j, rank)
    sampled = jnp.einsum("ajs,jal->jsl", z_all, stacked, preferred_element_type=WIDE)
    high = sampled.astype(NARROW)
    low = (sampled - high.astype(WIDE)).astype(NARROW)
    both = jnp.concatenate([high, low], axis=1)
    cross = jnp.einsum("jsl,jal->jsa", both, stacked, preferred_element_type=WIDE)
    cross = cross[:, :rank] + cross[:, rank:]
    gram = jnp.einsum("jsl,jtl->jst", sampled, sampled, precision=HIGHEST) / total
    inverse, cross = factor_over_inner(gram, cross, n_in)
    basis = jnp.einsum("jst,jtl->jsl", inverse, sampled, precision=HIGHEST)
    projected = jnp.einsum("jst,jta->jsa", inverse, cross, precision=HIGHEST) / math.sqrt(total)
    p_high = projected.astype(NARROW)
    p_low = (projected - p_high.astype(WIDE)).astype(NARROW)
    yk = yi.reshape(n_in * slots, own_j, rank, share)
    p_both = jnp.concatenate([p_high, p_low], axis=1).reshape(own_j, 2 * rank, n_in * slots, rank)
    coupling = jnp.einsum("jskr,kjrl->jsl", p_both, yk, preferred_element_type=WIDE)
    coupling = coupling[:, :rank] + coupling[:, rank:]
    return (basis[None], coupling[None])


def solution(mesh):
    sizes = (mesh.shape["row"], mesh.shape["col"], mesh.shape["inner"])
    in_specs = (
        P("row", "inner"),
        P("row", "inner", None, "col"),
        P("row", "inner", None, "col"),
        P("row", "inner", None, "col"),
        P("inner", "col", None, "row"),
        P("inner", "col", None, "row"),
        P("col", None, None),
    )
    out_specs = (P("row", "col", None, "inner"), P("row", "col", None, "inner"))
    return jax.shard_map(
        functools.partial(local, sizes), mesh=mesh, in_specs=in_specs, out_specs=out_specs, check_vma=False
    )
```
